512 devices in a mesh: section: 16 (over y, x), seq: 8 (over z_lo, core), dp: 4 (over z_hi).
Axes of the slice: x: 4, y: 4, z: 16 (z_hi: 4, z_lo: 4; z = z_hi * 4 + z_lo), core: 2. Of those that a mesh axis runs over, the one named last changes fastest.
Arguments:
- stream: bfloat16 [16, 4, 1024, 1280], P('section', 'dp', 'seq'), may hold values from -16 to 16
- norm_gain: float32 [16, 1280], P('section'), may hold values from 0.25 to 1.75
- w_xbc: bfloat16 [16, 1280, 2688], P('section', ('seq', 'dp')), may hold values from -0.15625 to 0.15625
- w_dt: bfloat16 [16, 1280, 40], P('section', ('seq', 'dp')), may hold values from -0.15625 to 0.15625
- conv_weight: float32 [16, 4, 2688], P('section'), may hold values from -3 to 3
- conv_bias: float32 [16, 2688], P('section'), may hold values from -1.8 to 1.8
- dt_bias: float32 [16, 40], P('section'), may hold values from -1 to 1
- decay_rate: float32 [16, 40], P('section'), may hold values from 9.765625e-05 to 0.04
- skip_weight: float32 [16, 40], P('section'), may hold values from 0.5 to 1.5
- inner_gain: float32 [16, 2560], P('section'), may hold values from 0.25 to 1.75
- w_out: bfloat16 [16, 2560, 1280], P('section', ('seq', 'dp')), may hold values from -0.125 to 0.125
Outputs:
- next_stream: bfloat16 [16, 4, 1024, 1280], P('section', 'dp', 'seq')
The draws below stay inside these ranges and needn't reach their ends.
All inputs are finite; a program needn't handle non-finite values.
Results may differ from the reference program's by a relative error of at most 0.008.
Values may be sent and summed in bfloat16 or wider, within the bound.
No kernel may reach another device: no remote copies, remote signals or barrier semaphores. Data moves between devices by JAX's collectives and lax.ppermute only.
A program may use at most 64 MiB of HBM per device.

```python
import math
import jax
import jax.numpy as jnp
from jax import lax

D = 1280
HEADS = 40
HEAD_DIM = 64
STATE = 64
CONV = 4
BLOCK = 128
INNER = 2560
CH = 2688
LENGTH = 1024
N_SECTION = 16
N_DP = 4


def draw_stream(key, part):
    base_key, row_key, col_key = jax.random.split(key, 3)
    full_shape = (N_SECTION, N_DP, LENGTH, D)
    row_scale = 10.0 ** jax.random.uniform(row_key, (N_SECTION, N_DP, LENGTH, 1), minval=-0.8, maxval=0.2)
    col_scale = 10.0 ** jax.random.uniform(col_key, (1, 1, 1, D), minval=-0.25, maxval=0.25)
    base_values = jax.random.normal(base_key, full_shape)
    return jnp.clip(base_values * row_scale * col_scale, -16.0, 16.0).astype(jnp.bfloat16)


def block_scale(stream_key, extent, cuts, low, high):
    level = 1.0
    for position, shards_of in cuts:
        steps = jax.random.uniform(jax.random.fold_in(jax.random.fold_in(stream_key, 6), position), (shards_of,), jnp.float32, low / len(cuts), high / len(cuts))
        level = level * jnp.repeat(jnp.exp(steps), extent[position] // shards_of).reshape((-1,) + (1,) * (len(extent) - 1 - position))
    return level


def centred(key, shape, deviation, reach, cuts=(), held_as=jnp.bfloat16):
    entries = jax.random.normal(key, shape, jnp.float32) * deviation
    if len(cuts) > 0:
        entries = block_scale(key, shape, cuts, -0.22, 0.18) * entries
    return jnp.clip(entries, min=-reach, max=reach).astype(held_as)


def setup_inputs(seed: int = 0) -> dict:
    key_list = jax.random.split(jax.random.key(seed), 12)
    return {
        "stream": draw_stream(jax.random.fold_in(key_list[11], 71), 0),
        "norm_gain": jnp.clip(1.0 + 0.15 * jax.random.normal(key_list[1], (N_SECTION, D), jnp.float32), 0.25, 1.75),
        "w_xbc": centred(key_list[2], (N_SECTION, D, CH), D ** -0.5, 0.15625, ((0, 16), (1, 32))),
        "w_dt": centred(key_list[3], (N_SECTION, D, HEADS), D ** -0.5, 0.15625, ((0, 16), (1, 32))),
        "conv_weight": centred(key_list[4], (N_SECTION, CONV, CH), CONV ** -0.5, 3.0, ((0, 16),), jnp.float32),
        "conv_bias": centred(key_list[5], (N_SECTION, CH), 0.3, 1.8, ((0, 16),), jnp.float32),
        "dt_bias": jnp.clip(jax.random.uniform(key_list[6], (N_SECTION, HEADS), jnp.float32, -1.0, 1.0) * block_scale(key_list[6], (N_SECTION, HEADS), ((0, 16),), -0.4, 0.0), -1.0, 1.0),
        "decay_rate": jnp.clip(jnp.exp(math.log(0.04) - 6.015181 * jax.random.uniform(key_list[7], (N_SECTION, HEADS), jnp.float32) ** block_scale(key_list[7], (N_SECTION, HEADS), ((0, 16),), -0.2, 0.2)), 9.765625145519152e-05, 0.04),
        "skip_weight": jnp.clip(0.5 + 1.0 * jax.random.uniform(key_list[8], (N_SECTION, HEADS), jnp.float32) ** block_scale(key_list[8], (N_SECTION, HEADS), ((0, 16),), -0.2, 0.2), 0.5, 1.5),
        "inner_gain": jnp.clip(1.0 + 0.15 * jax.random.normal(key_list[9], (N_SECTION, INNER), jnp.float32), 0.25, 1.75),
        "w_out": centred(key_list[10], (N_SECTION, INNER, D), INNER ** -0.5, 0.125, ((0, 16), (1, 32))),
    }


epsilon = 1e-05

def rms_scale(values, scale_gain):
    mean_square = lax.optimization_barrier(jnp.mean(values * values, axis=-1, keepdims=True))
    return values * lax.rsqrt(mean_square + epsilon) * scale_gain

def block_terms(values, b_rows, c_rows, dt_rows, head_rates):
    block_len = dt_rows.shape[0]
    cum_decay = jnp.cumsum(-dt_rows * head_rates[None, :], axis=0)
    scores = jnp.dot(c_rows, b_rows.T, preferred_element_type=jnp.float32)
    lag_decay = cum_decay.T[:, :, None] - cum_decay.T[:, None, :]
    causal = jnp.arange(block_len)[:, None] >= jnp.arange(block_len)[None, :]
    weights = jnp.where(causal[None], jnp.exp(jnp.minimum(lag_decay, 0.0)), 0.0)
    mixing = (scores[None] * weights * dt_rows.T[:, None, :]).astype(jnp.bfloat16)
    intra_out = jnp.einsum('hij,jhp->ihp', mixing.astype(jnp.float32), values.astype(jnp.float32))
    tail_weight = jnp.exp(cum_decay[-1][None, :] - cum_decay) * dt_rows
    scaled = (values.astype(jnp.float32) * tail_weight[:, :, None]).astype(jnp.bfloat16)
    summary = jnp.einsum('jhp,jn->hpn', scaled.astype(jnp.float32), b_rows.astype(jnp.float32))
    return (intra_out, summary, jnp.exp(cum_decay[-1]), jnp.exp(cum_decay))

def state_output(c_rows, growth, carried):
    readout = jnp.einsum('in,hpn->ihp', c_rows.astype(jnp.float32), carried, precision=lax.Precision.HIGHEST)
    return growth[:, :, None] * readout

def mamba_layer(seq_rows, row_gain, xbc_weight, dt_weight, tap_weight, tap_bias, dt_shift, head_rates, skip_gain, out_gain, out_weight):
    length_all = seq_rows.shape[0]
    blocks = length_all // BLOCK
    normed = rms_scale(seq_rows.astype(jnp.float32), row_gain).astype(jnp.bfloat16)
    xbc_raw = jnp.dot(normed, xbc_weight, preferred_element_type=jnp.float32).astype(jnp.bfloat16)
    dt_raw = jnp.dot(normed, dt_weight, preferred_element_type=jnp.float32)
    padded = jnp.concatenate([jnp.zeros((CONV - 1, xbc_raw.shape[1]), jnp.bfloat16), xbc_raw], axis=0)
    conv_sum = jnp.broadcast_to(tap_bias[None, :], xbc_raw.shape)
    for tap_index in range(CONV):
        conv_sum = conv_sum + tap_weight[tap_index][None, :] * padded[tap_index:tap_index + length_all].astype(jnp.float32)
    mixed_rows = jax.nn.silu(conv_sum).astype(jnp.bfloat16)
    values = mixed_rows[:, :INNER].reshape(blocks, BLOCK, HEADS, HEAD_DIM)
    b_rows = mixed_rows[:, INNER:INNER + STATE].reshape(blocks, BLOCK, STATE)
    c_rows = mixed_rows[:, INNER + STATE:].reshape(blocks, BLOCK, STATE)
    dt_rows = jax.nn.softplus(dt_raw + dt_shift[None, :]).reshape(blocks, BLOCK, HEADS)

    def block_step(carried, inputs):
        block_values, block_b, block_c, block_dt = inputs
        intra_out, summary, block_total, growth = block_terms(block_values, block_b, block_c, block_dt, head_rates)
        state_part = state_output(block_c, growth, carried)
        output = intra_out + state_part + skip_gain[None, :, None] * block_values.astype(jnp.float32)
        return (block_total[:, None, None] * carried + summary, output)
    zero_state = jnp.zeros((HEADS, HEAD_DIM, STATE), jnp.float32)
    final_state, outputs = lax.scan(block_step, zero_state, (values, b_rows, c_rows, dt_rows))
    normed_out = rms_scale(outputs.reshape(length_all, INNER), out_gain).astype(jnp.bfloat16)
    branch_out = jnp.dot(normed_out, out_weight, preferred_element_type=jnp.float32)
    return (seq_rows.astype(jnp.float32) + branch_out).astype(jnp.bfloat16)

def reference(stream, norm_gain, w_xbc, w_dt, conv_weight, conv_bias, dt_bias, decay_rate, skip_weight, inner_gain, w_out):

    def one_section(section_inputs):
        rows_all, row_gain, xbc_weight, dt_weight, tap_weight, tap_bias, dt_shift, head_rates, skip_gain, out_gain, out_weight = section_inputs

        def one_sequence(seq_rows):
            return mamba_layer(seq_rows, row_gain, xbc_weight, dt_weight, tap_weight, tap_bias, dt_shift, head_rates, skip_gain, out_gain, out_weight)
        return lax.map(one_sequence, rows_all)
    results = lax.map(one_section, (stream, norm_gain, w_xbc, w_dt, conv_weight, conv_bias, dt_bias, decay_rate, skip_weight, inner_gain, w_out))
    return jnp.roll(results, 1, axis=0)
```

```python
import functools

import jax
import jax.numpy as jnp
from jax import lax
from jax.experimental import pallas as pl
from jax.experimental.pallas import tpu as pltpu
from jax.sharding import Mesh
from jax.sharding import PartitionSpec as P

HEADS = 40
HEAD_DIM = 64
STATE = 64
CONV = 4
BLOCK = 128
INNER = 2560
D = 1280
SEQ = ("blk", "par", "core")
SEQ_DP = ("blk", "par", "core", "dp")
RING = ("blk", "dp")
epsilon = 1e-05
LOCAL_HEADS = 10
LOCAL = LOCAL_HEADS * HEAD_DIM
TAPPED = LOCAL + 2 * STATE
WIDE = TAPPED + 128
ROWS = 512
PIECE = ROWS // BLOCK


def ring_index(place):
    place = place % 8
    return (place % 2) * 4 + place // 2


def shifted(x, by):
    return lax.ppermute(x, RING, [(ring_index(i), ring_index(i + by)) for i in range(8)])


def gathered(x, cut):
    up, down = x, x
    out = [x]
    for _ in range(3):
        up, down = shifted(up, 1), shifted(down, -1)
        out += [up, down]
    half = x.shape[cut] // 2
    first = lax.slice_in_dim(up, 0, half, axis=cut)
    second = lax.slice_in_dim(down, half, 2 * half, axis=cut)
    out += [shifted(first, 1), shifted(second, -1)]
    return out


OFFSETS = (0, -1, 1, -2, 2, -3, 3, 4, 4)


def slot_of(place, offset):
    there = (place + offset + 8) % 8
    return (there % 2) * 4 + there // 2


def fill(place, chunks, scratch, cut):
    rows = chunks[0].shape[0]
    for k in range(7):
        at = pl.multiple_of(slot_of(place, OFFSETS[k]) * rows, 16)
        scratch[pl.ds(at, rows), :] = chunks[k][...]
    at = slot_of(place, 4) * rows
    if cut == 0:
        half = rows // 2
        scratch[pl.ds(pl.multiple_of(at, 16), half), :] = chunks[7][...]
        scratch[pl.ds(pl.multiple_of(at + half, 16), half), :] = chunks[8][...]
    else:
        half = chunks[7].shape[1]
        at = pl.multiple_of(at, 16)
        scratch[pl.ds(at, rows), :half] = chunks[7][...]
        scratch[pl.ds(at, rows), half:] = chunks[8][...]


def exact_dot(a, b):
    return jnp.dot(a, b, preferred_element_type=jnp.float32, precision=lax.Precision.HIGHEST)


def spread(per_head):
    rows = per_head.shape[0]
    left = lax.broadcasted_iota(jnp.int32, (rows, 128), 1) < HEAD_DIM
    pairs = []
    for p in range(LOCAL_HEADS // 2):
        first = jnp.broadcast_to(per_head[:, 2 * p : 2 * p + 1], (rows, 128))
        second = jnp.broadcast_to(per_head[:, 2 * p + 1 : 2 * p + 2], (rows, 128))
        pairs.append(jnp.where(left, first, second))
    return jnp.concatenate(pairs, axis=1)


def mix_kernel(place, rows, halo, taps, bias, dt_bias, rate, skip, *rest):
    chunks, (y_out, c_out, grown_out, state_out, weight, raw) = rest[:9], rest[9:]
    fill(place[0], chunks, weight, 0)
    projected = jnp.dot(rows[...], weight[...], preferred_element_type=jnp.float32)
    before = jnp.dot(halo[...], weight[:, :TAPPED], preferred_element_type=jnp.float32)
    raw[:8, :] = before.astype(jnp.bfloat16).astype(jnp.float32)
    raw[8:, :] = projected[:, :TAPPED].astype(jnp.bfloat16).astype(jnp.float32)
    shift = projected[:, TAPPED:] + dt_bias[...]
    dt_all = jnp.maximum(shift, 0.0) + jnp.log1p(jnp.exp(-jnp.abs(shift)))
    row_id = lax.broadcasted_iota(jnp.int32, (BLOCK, BLOCK), 0)
    col_id = lax.broadcasted_iota(jnp.int32, (BLOCK, BLOCK), 1)
    causal = row_id >= col_id
    lower = causal.astype(jnp.float32)
    left = col_id < HEAD_DIM
    state = jnp.zeros((STATE, LOCAL), jnp.float32)
    decayed = jnp.ones((1, LOCAL), jnp.float32)
    for n in range(PIECE):
        at = n * BLOCK
        conv = bias[...] + taps[0:1, :] * raw[at + 5 : at + 5 + BLOCK, :]
        for k in range(1, CONV):
            conv = conv + taps[k : k + 1, :] * raw[at + 5 + k : at + 5 + k + BLOCK, :]
        xbc = (conv / (1.0 + jnp.exp(-conv))).astype(jnp.bfloat16)
        values = xbc[:, :LOCAL]
        both = xbc[:, LOCAL:]
        b_rows, c_rows = both[:, :STATE], both[:, STATE:]
        dt = dt_all[at : at + BLOCK, :]
        cum = exact_dot(lower, -dt * rate[...])
        cum_t, dt_t = cum.T, dt.T
        scores = lax.dot_general(
            c_rows, b_rows, (((1,), (1,)), ((), ())), preferred_element_type=jnp.float32
        )
        scores = jnp.where(causal, scores, 0.0)
        intra = []
        for p in range(LOCAL_HEADS // 2):
            mixes = []
            for h in (2 * p, 2 * p + 1):
                lag = cum[:, h : h + 1] - cum_t[h : h + 1, :]
                weights = jnp.exp(jnp.minimum(lag, 0.0))
                mixes.append((scores * weights * dt_t[h : h + 1, :]).astype(jnp.bfloat16))
            pair = values[:, 128 * p : 128 * p + 128]
            none = jnp.zeros_like(pair)
            stacked = jnp.concatenate(
                [jnp.where(left, pair, none), jnp.where(left, none, pair)], axis=0
            )
            intra.append(
                jnp.dot(
                    jnp.concatenate(mixes, axis=1), stacked, preferred_element_type=jnp.float32
                )
            )
        wide = values.astype(jnp.float32)
        tail = spread(jnp.exp(cum[BLOCK - 1 :, :] - cum) * dt)
        growth = spread(jnp.exp(cum))
        scaled = (wide * tail).astype(jnp.bfloat16)
        local = jnp.concatenate(intra, axis=1) + skip[...] * wide
        if n > 0:
            local = local + growth * exact_dot(c_rows.astype(jnp.float32), state)
        y_out[at : at + BLOCK, :] = local
        c_out[at : at + BLOCK, :] = c_rows
        grown_out[at : at + BLOCK, :] = growth * decayed
        summary = lax.dot_general(
            b_rows, scaled, (((0,), (0,)), ((), ())), preferred_element_type=jnp.float32
        )
        total = growth[BLOCK - 1 :, :]
        state = total * state + summary
        decayed = decayed * total
    state_out[...] = state.astype(jnp.bfloat16)


def late_kernel(y_in, c_in, grown, arriving, y_out, square_out):
    y = y_in[...] + grown[...] * jnp.dot(
        c_in[...], arriving[...], preferred_element_type=jnp.float32
    )
    y_out[...] = y
    square_out[...] = jnp.broadcast_to(jnp.sum(y * y, axis=1, keepdims=True), (ROWS, 128))


def out_kernel(place, y_in, square, gain, *rest):
    chunks, (out, weight) = rest[:9], rest[9:]
    fill(place[0], chunks, weight, 1)
    scale = lax.rsqrt(square[:, :1] * (1.0 / INNER) + epsilon)
    normed = (y_in[...] * scale * gain[...]).astype(jnp.bfloat16)
    out[...] = jnp.dot(normed, weight[...], preferred_element_type=jnp.float32).astype(jnp.bfloat16)


VMEM = pl.BlockSpec(memory_space=pltpu.VMEM)
SMEM = pl.BlockSpec(memory_space=pltpu.SMEM)


def call(kernel, outs, scratch, scalars, *arrays):
    return pl.pallas_call(
        kernel,
        out_shape=outs,
        in_specs=[SMEM] * len(scalars) + [VMEM] * len(arrays),
        out_specs=jax.tree.map(lambda _: VMEM, outs),
        scratch_shapes=scratch,
        compiler_params=pltpu.CompilerParams(vmem_limit_bytes=40 * 1024 * 1024),
    )(*scalars, *arrays)


def swapped(x, axis):
    return lax.ppermute(x, axis, [(0, 1), (1, 0)])


def both_of(mine, theirs, index):
    first = jnp.where(index == 0, mine, theirs)
    second = jnp.where(index == 0, theirs, mine)
    return jnp.stack([first, second])


def of_class(x, group, width):
    lead = x.shape[:-1]
    picked = lax.dynamic_index_in_dim(x.reshape(*lead, 2, 4, width), group, len(lead) + 1, False)
    return picked.reshape(*lead, 2 * width)


def shards(
    stream,
    norm_gain,
    w_xbc,
    w_dt,
    conv_weight,
    conv_bias,
    dt_bias,
    decay_rate,
    skip_weight,
    inner_gain,
    w_out,
):
    par, core = lax.axis_index("par"), lax.axis_index("core")
    group = par * 2 + core
    place = (lax.axis_index("dp") * 2 + lax.axis_index("blk")).astype(jnp.int32).reshape(1)

    out_chunks = gathered(w_out[0], 1)
    xbc, dtw = w_xbc[0], w_dt[0]
    inner = xbc[:, :INNER].reshape(40, 2, 4, 320).transpose(2, 0, 1, 3).reshape(4, 40, LOCAL)
    shared = jnp.broadcast_to(xbc[None, :, INNER:], (4, 40, 2 * STATE))
    steps = dtw.reshape(40, 2, 4, 5).transpose(2, 0, 1, 3).reshape(4, 40, LOCAL_HEADS)
    steps = jnp.pad(steps, ((0, 0), (0, 0), (0, 128 - LOCAL_HEADS)))
    packed = jnp.concatenate([inner, shared, steps], axis=2)
    classes = lax.all_to_all(packed, ("par", "core"), 0, 0).reshape(160, WIDE)
    in_chunks = gathered(classes, 0)

    rows_in = stream[0, 0]
    wide = rows_in.astype(jnp.float32)
    mean_square = jnp.mean(wide * wide, axis=-1, keepdims=True)
    normed = (wide * lax.rsqrt(mean_square + epsilon) * norm_gain[0]).astype(jnp.bfloat16)
    feature = lax.broadcasted_iota(jnp.int32, (D, D), 0)
    target = lax.broadcasted_iota(jnp.int32, (D, D), 1)
    source = (target // 640) * 640 + (target // 40 % 4) * 160 + (target // 160 % 4) * 40 + target % 40
    select = (feature == source).astype(jnp.bfloat16)
    normed = jnp.dot(normed, select, preferred_element_type=jnp.float32).astype(jnp.bfloat16)
    pair = both_of(normed, swapped(normed, "par"), par)
    quad = both_of(pair, swapped(pair, "core"), core)
    rows = quad.transpose(1, 0, 2, 3).reshape(ROWS, D)
    halo = lax.ppermute(rows[ROWS - 8 :], "blk", [(0, 1)])

    taps = conv_weight[0]
    taps = jnp.concatenate([of_class(taps[:, :INNER], group, 320), taps[:, INNER:]], axis=1)
    tap_bias = conv_bias[0][None]
    tap_bias = jnp.concatenate([of_class(tap_bias[:, :INNER], group, 320), tap_bias[:, INNER:]], axis=1)
    per_head = [of_class(p, group, 5) for p in (dt_bias, decay_rate, skip_weight)]
    shift, rate = (jnp.pad(p, ((0, 0), (0, 128 - LOCAL_HEADS))) for p in per_head[:2])
    skip = jnp.repeat(per_head[2], HEAD_DIM, axis=1)
    gain = of_class(inner_gain, group, 320)

    f32, bf16 = jnp.float32, jnp.bfloat16
    y_local, c_rows, grown, state = call(
        mix_kernel,
        (
            jax.ShapeDtypeStruct((ROWS, LOCAL), f32),
            jax.ShapeDtypeStruct((ROWS, STATE), bf16),
            jax.ShapeDtypeStruct((ROWS, LOCAL), f32),
            jax.ShapeDtypeStruct((STATE, LOCAL), bf16),
        ),
        [pltpu.VMEM((D, WIDE), bf16), pltpu.VMEM((ROWS + 8, TAPPED), f32)],
        (place,),
        rows,
        halo,
        taps,
        tap_bias,
        shift,
        rate,
        skip,
        *in_chunks,
    )
    arriving = lax.ppermute(state, "blk", [(0, 1)])
    y, square = call(
        late_kernel,
        (jax.ShapeDtypeStruct((ROWS, LOCAL), f32), jax.ShapeDtypeStruct((ROWS, 128), f32)),
        [],
        (),
        y_local,
        c_rows,
        grown,
        arriving,
    )
    square = square[:, 0].reshape(PIECE, BLOCK)
    square = square + swapped(square, "core")
    square = square + swapped(square, "par")
    square = jnp.broadcast_to(square.reshape(ROWS, 1), (ROWS, 128))
    partial = call(
        out_kernel,
        jax.ShapeDtypeStruct((ROWS, D), bf16),
        [pltpu.VMEM((LOCAL, D), bf16)],
        (place,),
        y,
        square,
        gain,
        *out_chunks,
    ).reshape(2, 2, BLOCK, D)

    own = jnp.where(core == 0, partial[:, 0], partial[:, 1])
    other = jnp.where(core == 0, partial[:, 1], partial[:, 0])
    chip = own.astype(f32) + swapped(other, "core").astype(f32)
    own = jnp.where(par == 0, chip[0], chip[1])
    other = jnp.where(par == 0, chip[1], chip[0]).astype(bf16)
    branch = own + swapped(other, "par").astype(f32)
    next_rows = (wide + branch).astype(bf16)
    moved = lax.ppermute(next_rows, "section", [(i, (i + 1) % 16) for i in range(16)])
    return moved[None, None]


def solution(mesh):
    torus = Mesh(
        mesh.devices.reshape(mesh.shape["section"], 2, 2, 2, mesh.shape["dp"]),
        ("section", "blk", "par", "core", "dp"),
    )
    return jax.shard_map(
        shards,
        mesh=torus,
        in_specs=(
            P("section", "dp", SEQ, None),
            P("section", None),
            P("section", SEQ_DP, None),
            P("section", SEQ_DP, None),
            P("section", None, None),
            P("section", None),
            P("section", None),
            P("section", None),
            P("section", None),
            P("section", None),
            P("section", SEQ_DP, None),
        ),
        out_specs=P("section", "dp", SEQ, None),
        check_vma=False,
    )
```

```python
import jax
import jax.numpy as jnp
from jax import lax
from jax.experimental import pallas as pl
from jax.experimental.pallas import tpu as pltpu
from jax.sharding import Mesh
from jax.sharding import PartitionSpec as P

HEADS = 40
HEAD_DIM = 64
STATE = 64
CONV = 4
BLOCK = 128
INNER = 2560
D = 1280
SEQ = ("blk", "par", "core")
SEQ_DP = ("blk", "par", "core", "dp")
RING = ("blk", "core", "dp")
epsilon = 1e-05
LOCAL_HEADS = 10
LOCAL = LOCAL_HEADS * HEAD_DIM
TAPPED = LOCAL + 2 * STATE
WIDE = TAPPED + 128
ROWS = 512
PIECE = ROWS // BLOCK


def ring_index(place, core):
    place = place % 8
    return (place % 2) * 8 + core * 4 + place // 2


def shifted(x, by):
    pairs = []
    for i in range(8):
        pairs.append((ring_index(i, 0), ring_index(i + by, 0)))
        pairs.append((ring_index(i, 1), ring_index(i - by, 1)))
    return lax.ppermute(x, RING, pairs)


def gathered(x, cut):
    up, down = x, x
    out = [x]
    for _ in range(1, 4):
        up, down = shifted(up, 1), shifted(down, -1)
        out += [up, down]
    half = x.shape[cut] // 2
    first = lax.slice_in_dim(up, 0, half, axis=cut)
    second = lax.slice_in_dim(down, half, 2 * half, axis=cut)
    out += [shifted(first, 1), shifted(second, -1)]
    return out


OFFSETS = (0, -1, 1, -2, 2, -3, 3, 4, 4)


def slot_of(place, offset):
    there = (place + offset + 8) % 8
    return (there % 2) * 4 + there // 2


def fill(where, chunks, scratch, cut):
    rows = chunks[0].shape[0]
    place, sign = where[0], where[1]
    for k in range(7):
        at = pl.multiple_of(slot_of(place, OFFSETS[k] * sign) * rows, 16)
        scratch[pl.ds(at, rows), :] = chunks[k][...]
    at = slot_of(place, 4) * rows
    if cut == 0:
        half = rows // 2
        scratch[pl.ds(pl.multiple_of(at, 16), half), :] = chunks[7][...]
        scratch[pl.ds(pl.multiple_of(at + half, 16), half), :] = chunks[8][...]
    else:
        half = chunks[7].shape[1]
        at = pl.multiple_of(at, 16)
        scratch[pl.ds(at, rows), :half] = chunks[7][...]
        scratch[pl.ds(at, rows), half:] = chunks[8][...]


def exact_dot(a, b):
    return jnp.dot(a, b, preferred_element_type=jnp.float32, precision=lax.Precision.HIGHEST)


def spread(per_head):
    rows = per_head.shape[0]
    left = lax.broadcasted_iota(jnp.int32, (rows, 128), 1) < HEAD_DIM
    pairs = []
    for p in range(LOCAL_HEADS // 2):
        first = jnp.broadcast_to(per_head[:, 2 * p : 2 * p + 1], (rows, 128))
        second = jnp.broadcast_to(per_head[:, 2 * p + 1 : 2 * p + 2], (rows, 128))
        pairs.append(jnp.where(left, first, second))
    return jnp.concatenate(pairs, axis=1)


def class_columns(x, group, width):
    found = None
    for g in range(4):
        piece = jnp.concatenate(
            [x[:, g * width : (g + 1) * width], x[:, (g + 4) * width : (g + 5) * width]], axis=1
        )
        found = piece if found is None else jnp.where(group == g, piece, found)
    return found


def class_heads(x, group, width, lanes):
    head = lax.broadcasted_iota(jnp.int32, (HEADS, lanes), 0)
    local = lax.broadcasted_iota(jnp.int32, (HEADS, lanes), 1) // width
    wanted = jnp.where(local < 5, group * 5 + local, 15 + group * 5 + local)
    select = jnp.logical_and(local < LOCAL_HEADS, head == wanted)
    return exact_dot(x, select.astype(jnp.float32))


def mix_kernel(where, rows, halo, all_taps, all_bias, all_dt_bias, all_rate, all_skip, *rest):
    chunks, (y_out, c_out, grown_out, state_out, weight, raw) = rest[:9], rest[9:]
    fill(where, chunks, weight, 0)
    group = where[2]
    taps = jnp.concatenate(
        [class_columns(all_taps[0], group, 320), all_taps[0, :, INNER:]], axis=1
    )
    bias = jnp.concatenate(
        [class_columns(all_bias[...], group, 320), all_bias[:, INNER:]], axis=1
    )
    dt_bias = class_heads(all_dt_bias[...], group, 1, 128)
    rate = class_heads(all_rate[...], group, 1, 128)
    skip = class_heads(all_skip[...], group, HEAD_DIM, LOCAL)
    projected = jnp.dot(rows[...], weight[...], preferred_element_type=jnp.float32)
    before = jnp.dot(halo[...], weight[:, :TAPPED], preferred_element_type=jnp.float32)
    raw[:8, :] = before.astype(jnp.bfloat16).astype(jnp.float32)
    raw[8:, :] = projected[:, :TAPPED].astype(jnp.bfloat16).astype(jnp.float32)
    shift = projected[:, TAPPED:] + dt_bias
    dt_all = jnp.maximum(shift, 0.0) + jnp.log1p(jnp.exp(-jnp.abs(shift)))
    row_id = lax.broadcasted_iota(jnp.int32, (BLOCK, BLOCK), 0)
    col_id = lax.broadcasted_iota(jnp.int32, (BLOCK, BLOCK), 1)
    causal = row_id >= col_id
    lower = causal.astype(jnp.float32)
    left = col_id < HEAD_DIM
    state = jnp.zeros((STATE, LOCAL), jnp.float32)
    decayed = jnp.ones((1, LOCAL), jnp.float32)
    for n in range(PIECE):
        at = n * BLOCK
        conv = bias + taps[0:1, :] * raw[at + 5 : at + 5 + BLOCK, :]
        for k in range(1, CONV):
            conv = conv + taps[k : k + 1, :] * raw[at + 5 + k : at + 5 + k + BLOCK, :]
        xbc = (conv / (1.0 + jnp.exp(-conv))).astype(jnp.bfloat16)
        values = xbc[:, :LOCAL]
        both = xbc[:, LOCAL:]
        b_rows, c_rows = both[:, :STATE], both[:, STATE:]
        dt = dt_all[at : at + BLOCK, :]
        cum = exact_dot(lower, -dt * rate)
        cum_t, dt_t = cum.T, dt.T
        scores = lax.dot_general(
            c_rows, b_rows, (((1,), (1,)), ((), ())), preferred_element_type=jnp.float32
        )
        scores = jnp.where(causal, scores, 0.0)
        intra = []
        for p in range(LOCAL_HEADS // 2):
            mixes = []
            for h in (2 * p, 2 * p + 1):
                lag = cum[:, h : h + 1] - cum_t[h : h + 1, :]
                weights = jnp.exp(jnp.minimum(lag, 0.0))
                mixes.append((scores * weights * dt_t[h : h + 1, :]).astype(jnp.bfloat16))
            pair = values[:, 128 * p : 128 * p + 128]
            none = jnp.zeros_like(pair)
            stacked = jnp.concatenate(
                [jnp.where(left, pair, none), jnp.where(left, none, pair)], axis=0
            )
            intra.append(
                jnp.dot(
                    jnp.concatenate(mixes, axis=1), stacked, preferred_element_type=jnp.float32
                )
            )
        wide = values.astype(jnp.float32)
        tail = spread(jnp.exp(cum[BLOCK - 1 :, :] - cum) * dt)
        growth = spread(jnp.exp(cum))
        scaled = (wide * tail).astype(jnp.bfloat16)
        local = jnp.concatenate(intra, axis=1) + skip * wide
        if n > 0:
            local = local + growth * exact_dot(c_rows.astype(jnp.float32), state)
        y_out[at : at + BLOCK, :] = local
        c_out[at : at + BLOCK, :] = c_rows
        grown_out[at : at + BLOCK, :] = growth * decayed
        summary = lax.dot_general(
            b_rows, scaled, (((0,), (0,)), ((), ())), preferred_element_type=jnp.float32
        )
        total = growth[BLOCK - 1 :, :]
        state = total * state + summary
        decayed = decayed * total
    state_out[...] = state.astype(jnp.bfloat16)


def late_kernel(y_in, c_in, grown, arriving, y_out, square_out):
    y = y_in[...] + grown[...] * jnp.dot(
        c_in[...], arriving[...], preferred_element_type=jnp.float32
    )
    y_out[...] = y
    square_out[...] = jnp.broadcast_to(jnp.sum(y * y, axis=1, keepdims=True), (ROWS, 128))


def out_kernel(where, y_in, square, all_gain, *rest):
    chunks, (out, weight) = rest[:9], rest[9:]
    fill(where, chunks, weight, 1)
    gain = class_columns(all_gain[...], where[2], 320)
    scale = lax.rsqrt(square[:, :1] * (1.0 / INNER) + epsilon)
    normed = (y_in[...] * scale * gain).astype(jnp.bfloat16)
    out[...] = jnp.dot(normed, weight[...], preferred_element_type=jnp.float32).astype(jnp.bfloat16)


VMEM = pl.BlockSpec(memory_space=pltpu.VMEM)
SMEM = pl.BlockSpec(memory_space=pltpu.SMEM)


def call(kernel, outs, scratch, scalars, *arrays):
    return pl.pallas_call(
        kernel,
        out_shape=outs,
        in_specs=[SMEM] * len(scalars) + [VMEM] * len(arrays),
        out_specs=jax.tree.map(lambda _: VMEM, outs),
        scratch_shapes=scratch,
        compiler_params=pltpu.CompilerParams(vmem_limit_bytes=40 * 1024 * 1024),
    )(*scalars, *arrays)


def swapped(x, axis):
    return lax.ppermute(x, axis, [(0, 1), (1, 0)])


def both_of(mine, theirs, index):
    first = jnp.where(index == 0, mine, theirs)
    second = jnp.where(index == 0, theirs, mine)
    return jnp.stack([first, second])


def shards(
    stream,
    norm_gain,
    w_xbc,
    w_dt,
    conv_weight,
    conv_bias,
    dt_bias,
    decay_rate,
    skip_weight,
    inner_gain,
    w_out,
):
    par, core = lax.axis_index("par"), lax.axis_index("core")
    group = par * 2 + core
    place = lax.axis_index("dp") * 2 + lax.axis_index("blk")
    where = jnp.stack([place, 1 - 2 * core, group]).astype(jnp.int32)

    out_chunks = gathered(w_out[0], 1)
    xbc, dtw = w_xbc[0], w_dt[0]
    inner = xbc[:, :INNER].reshape(40, 2, 4, 320).transpose(2, 0, 1, 3).reshape(4, 40, LOCAL)
    shared = jnp.broadcast_to(xbc[None, :, INNER:], (4, 40, 2 * STATE))
    steps = dtw.reshape(40, 2, 4, 5).transpose(2, 0, 1, 3).reshape(4, 40, LOCAL_HEADS)
    steps = jnp.pad(steps, ((0, 0), (0, 0), (0, 128 - LOCAL_HEADS)))
    packed = jnp.concatenate([inner, shared, steps], axis=2)
    classes = lax.all_to_all(packed, ("par", "core"), 0, 0).reshape(160, WIDE)
    in_chunks = gathered(classes, 0)

    rows_in = stream[0, 0]
    wide = rows_in.astype(jnp.float32)
    mean_square = jnp.mean(wide * wide, axis=-1, keepdims=True)
    normed = (wide * lax.rsqrt(mean_square + epsilon) * norm_gain[0]).astype(jnp.bfloat16)
    feature = lax.broadcasted_iota(jnp.int32, (D, D), 0)
    target = lax.broadcasted_iota(jnp.int32, (D, D), 1)
    source = (target // 640) * 640 + (target // 40 % 4) * 160 + (target // 160 % 4) * 40 + target % 40
    select = (feature == source).astype(jnp.bfloat16)
    normed = jnp.dot(normed, select, preferred_element_type=jnp.float32).astype(jnp.bfloat16)
    pair = both_of(normed, swapped(normed, "par"), par)
    quad = both_of(pair, swapped(pair, "core"), core)
    rows = quad.transpose(1, 0, 2, 3).reshape(ROWS, D)
    halo = lax.ppermute(rows[ROWS - 8 :], "blk", [(0, 1)])

    f32, bf16 = jnp.float32, jnp.bfloat16
    y_local, c_rows, grown, state = call(
        mix_kernel,
        (
            jax.ShapeDtypeStruct((ROWS, LOCAL), f32),
            jax.ShapeDtypeStruct((ROWS, STATE), bf16),
            jax.ShapeDtypeStruct((ROWS, LOCAL), f32),
            jax.ShapeDtypeStruct((STATE, LOCAL), bf16),
        ),
        [pltpu.VMEM((D, WIDE), bf16), pltpu.VMEM((ROWS + 8, TAPPED), f32)],
        (where,),
        rows,
        halo,
        conv_weight,
        conv_bias,
        dt_bias,
        decay_rate,
        skip_weight,
        *in_chunks,
    )
    arriving = lax.ppermute(state, "blk", [(0, 1)])
    y, square = call(
        late_kernel,
        (jax.ShapeDtypeStruct((ROWS, LOCAL), f32), jax.ShapeDtypeStruct((ROWS, 128), f32)),
        [],
        (),
        y_local,
        c_rows,
        grown,
        arriving,
    )
    square = square[:, 0].reshape(PIECE, BLOCK)
    square = square + swapped(square, "core")
    square = square + swapped(square, "par")
    square = jnp.broadcast_to(square.reshape(ROWS, 1), (ROWS, 128))
    partial = call(
        out_kernel,
        jax.ShapeDtypeStruct((ROWS, D), bf16),
        [pltpu.VMEM((LOCAL, D), bf16)],
        (where,),
        y,
        square,
        inner_gain,
        *out_chunks,
    ).reshape(2, 2, BLOCK, D)

    own = jnp.where(core == 0, partial[:, 0], partial[:, 1])
    other = jnp.where(core == 0, partial[:, 1], partial[:, 0])
    chip = own.astype(f32) + swapped(other, "core").astype(f32)
    own = jnp.where(par == 0, chip[0], chip[1])
    other = jnp.where(par == 0, chip[1], chip[0]).astype(bf16)
    branch = own + swapped(other, "par").astype(f32)
    next_rows = (wide + branch).astype(bf16)
    moved = lax.ppermute(next_rows, "section", [(i, (i + 1) % 16) for i in range(16)])
    return moved[None, None]


def solution(mesh):
    torus = Mesh(
        mesh.devices.reshape(mesh.shape["section"], 2, 2, 2, mesh.shape["dp"]),
        ("section", "blk", "par", "core", "dp"),
    )
    return jax.shard_map(
        shards,
        mesh=torus,
        in_specs=(
            P("section", "dp", SEQ, None),
            P("section", None),
            P("section", SEQ_DP, None),
            P("section", SEQ_DP, None),
            P("section", None, None),
            P("section", None),
            P("section", None),
            P("section", None),
            P("section", None),
            P("section", None),
            P("section", SEQ_DP, None),
        ),
        out_specs=P("section", "dp", SEQ, None),
        check_vma=False,
    )
```

```python
import jax
import jax.numpy as jnp
from jax import lax
from jax.experimental import pallas as pl
from jax.experimental.pallas import tpu as pltpu
from jax.sharding import Mesh
from jax.sharding import PartitionSpec as P

HEADS = 40
HEAD_DIM = 64
STATE = 64
CONV = 4
BLOCK = 128
INNER = 2560
D = 1280
SEQ = ("blk", "par", "core")
SEQ_DP = ("blk", "par", "core", "dp")
RING = ("blk", "core", "dp")
epsilon = 1e-05
LOCAL_HEADS = 10
LOCAL = LOCAL_HEADS * HEAD_DIM
TAPPED = LOCAL + 2 * STATE
WIDE = TAPPED + 128
ROWS = 512
PIECE = ROWS // BLOCK
HALF = D // 2


def ring_index(place, core):
    place = place % 8
    return (place % 2) * 8 + core * 4 + place // 2


def shifted(x, by):
    pairs = []
    for i in range(8):
        pairs.append((ring_index(i, 0), ring_index(i + by, 0)))
        pairs.append((ring_index(i, 1), ring_index(i - by, 1)))
    return lax.ppermute(x, RING, pairs)


def gathered(x, cut):
    up, down = x, x
    out = [x]
    for _ in range(1, 4):
        up, down = shifted(up, 1), shifted(down, -1)
        out += [up, down]
    half = x.shape[cut] // 2
    first = lax.slice_in_dim(up, 0, half, axis=cut)
    second = lax.slice_in_dim(down, half, 2 * half, axis=cut)
    out += [shifted(first, 1), shifted(second, -1)]
    return out


OFFSETS = (0, -1, 1, -2, 2, -3, 3, 4, 4)


def slot_of(place, offset):
    there = (place + offset + 8) % 8
    return (there % 2) * 4 + there // 2


def fill(where, chunks, scratch, cut):
    rows = chunks[0].shape[0]
    place, sign = where[0], where[1]
    for k in range(7):
        at = pl.multiple_of(slot_of(place, OFFSETS[k] * sign) * rows, 16)
        scratch[pl.ds(at, rows), :] = chunks[k][...]
    at = slot_of(place, 4) * rows
    if cut == 0:
        half = rows // 2
        scratch[pl.ds(pl.multiple_of(at, 16), half), :] = chunks[7][...]
        scratch[pl.ds(pl.multiple_of(at + half, 16), half), :] = chunks[8][...]
    else:
        half = chunks[7].shape[1]
        at = pl.multiple_of(at, 16)
        scratch[pl.ds(at, rows), :half] = chunks[7][...]
        scratch[pl.ds(at, rows), half:] = chunks[8][...]


def exact_dot(a, b):
    return jnp.dot(a, b, preferred_element_type=jnp.float32, precision=lax.Precision.HIGHEST)


def spread(per_head):
    rows = per_head.shape[0]
    left = lax.broadcasted_iota(jnp.int32, (rows, 128), 1) < HEAD_DIM
    pairs = []
    for p in range(LOCAL_HEADS // 2):
        first = jnp.broadcast_to(per_head[:, 2 * p : 2 * p + 1], (rows, 128))
        second = jnp.broadcast_to(per_head[:, 2 * p + 1 : 2 * p + 2], (rows, 128))
        pairs.append(jnp.where(left, first, second))
    return jnp.concatenate(pairs, axis=1)


def class_columns(x, group, width):
    found = None
    for g in range(4):
        piece = jnp.concatenate(
            [x[:, g * width : (g + 1) * width], x[:, (g + 4) * width : (g + 5) * width]], axis=1
        )
        found = piece if found is None else jnp.where(group == g, piece, found)
    return found


def class_heads(x, group, width, lanes):
    head = lax.broadcasted_iota(jnp.int32, (HEADS, lanes), 0)
    local = lax.broadcasted_iota(jnp.int32, (HEADS, lanes), 1) // width
    wanted = jnp.where(local < 5, group * 5 + local, 15 + group * 5 + local)
    select = jnp.logical_and(local < LOCAL_HEADS, head == wanted)
    return exact_dot(x, select.astype(jnp.float32))


def mix_kernel(where, rows, halo, all_taps, all_bias, all_dt_bias, all_rate, all_skip, *rest):
    chunks, (y_out, c_out, grown_out, state_out, weight, raw) = rest[:9], rest[9:]
    fill(where, chunks, weight, 0)
    group = where[2]
    taps = jnp.concatenate(
        [class_columns(all_taps[0], group, 320), all_taps[0, :, INNER:]], axis=1
    )
    bias = jnp.concatenate(
        [class_columns(all_bias[...], group, 320), all_bias[:, INNER:]], axis=1
    )
    dt_bias = class_heads(all_dt_bias[...], group, 1, 128)
    rate = class_heads(all_rate[...], group, 1, 128)
    skip = class_heads(all_skip[...], group, HEAD_DIM, LOCAL)
    projected = jnp.dot(rows[...], weight[...], preferred_element_type=jnp.float32)
    before = jnp.dot(halo[...], weight[:, :TAPPED], preferred_element_type=jnp.float32)
    raw[:8, :] = before.astype(jnp.bfloat16).astype(jnp.float32)
    raw[8:, :] = projected[:, :TAPPED].astype(jnp.bfloat16).astype(jnp.float32)
    shift = projected[:, TAPPED:] + dt_bias
    dt_all = jnp.maximum(shift, 0.0) + jnp.log1p(jnp.exp(-jnp.abs(shift)))
    row_id = lax.broadcasted_iota(jnp.int32, (BLOCK, BLOCK), 0)
    col_id = lax.broadcasted_iota(jnp.int32, (BLOCK, BLOCK), 1)
    causal = row_id >= col_id
    lower = causal.astype(jnp.float32)
    left = col_id < HEAD_DIM
    state = jnp.zeros((STATE, LOCAL), jnp.float32)
    decayed = jnp.ones((1, LOCAL), jnp.float32)
    for n in range(PIECE):
        at = n * BLOCK
        conv = bias + taps[0:1, :] * raw[at + 5 : at + 5 + BLOCK, :]
        for k in range(1, CONV):
            conv = conv + taps[k : k + 1, :] * raw[at + 5 + k : at + 5 + k + BLOCK, :]
        xbc = (conv / (1.0 + jnp.exp(-conv))).astype(jnp.bfloat16)
        values = xbc[:, :LOCAL]
        both = xbc[:, LOCAL:]
        b_rows, c_rows = both[:, :STATE], both[:, STATE:]
        dt = dt_all[at : at + BLOCK, :]
        cum = exact_dot(lower, -dt * rate)
        cum_t, dt_t = cum.T, dt.T
        scores = lax.dot_general(
            c_rows, b_rows, (((1,), (1,)), ((), ())), preferred_element_type=jnp.float32
        )
        scores = jnp.where(causal, scores, 0.0)
        intra = []
        for p in range(LOCAL_HEADS // 2):
            mixes = []
            for h in (2 * p, 2 * p + 1):
                lag = cum[:, h : h + 1] - cum_t[h : h + 1, :]
                weights = jnp.exp(jnp.minimum(lag, 0.0))
                mixes.append((scores * weights * dt_t[h : h + 1, :]).astype(jnp.bfloat16))
            pair = values[:, 128 * p : 128 * p + 128]
            none = jnp.zeros_like(pair)
            stacked = jnp.concatenate(
                [jnp.where(left, pair, none), jnp.where(left, none, pair)], axis=0
            )
            intra.append(
                jnp.dot(
                    jnp.concatenate(mixes, axis=1), stacked, preferred_element_type=jnp.float32
                )
            )
        wide = values.astype(jnp.float32)
        tail = spread(jnp.exp(cum[BLOCK - 1 :, :] - cum) * dt)
        growth = spread(jnp.exp(cum))
        scaled = (wide * tail).astype(jnp.bfloat16)
        local = jnp.concatenate(intra, axis=1) + skip * wide
        if n > 0:
            local = local + growth * exact_dot(c_rows.astype(jnp.float32), state)
        y_out[at : at + BLOCK, :] = local
        c_out[at : at + BLOCK, :] = c_rows
        grown_out[at : at + BLOCK, :] = growth * decayed
        summary = lax.dot_general(
            b_rows, scaled, (((0,), (0,)), ((), ())), preferred_element_type=jnp.float32
        )
        total = growth[BLOCK - 1 :, :]
        state = total * state + summary
        decayed = decayed * total
    state_out[...] = state.astype(jnp.bfloat16)


def pieces(square, lane):
    high = square.astype(jnp.bfloat16).astype(jnp.float32)
    middle = (square - high).astype(jnp.bfloat16).astype(jnp.float32)
    low = square - high - middle
    split = jnp.where(lane == 0, high, jnp.where(lane == 1, middle, jnp.where(lane == 2, low, 0.0)))
    return split.astype(jnp.bfloat16)


def out_kernel(where, y_in, c_in, grown, arriving, all_gain, *rest):
    chunks, (keep_x, send_x, keep_y, send_y, weight, act, square, ordered) = rest[:9], rest[9:]
    fill(where, chunks, weight, 1)
    gain = class_columns(all_gain[...], where[2], 320)
    y = y_in[...] + grown[...] * jnp.dot(
        c_in[...], arriving[...], preferred_element_type=jnp.float32
    )
    act[...] = (y * gain).astype(jnp.bfloat16)
    square[...] = jnp.broadcast_to(jnp.sum(y * y, axis=1, keepdims=True), (ROWS, 128))
    par, core = where[3], where[4]
    starts = []
    for p in (par, 1 - par):
        for c in (core, 1 - core):
            starts.append(pl.multiple_of((p * 2 + c) * BLOCK, BLOCK))
    for k in range(4):
        ordered[k * BLOCK : (k + 1) * BLOCK, :] = act[pl.ds(starts[k], BLOCK), :]
    lane = lax.broadcasted_iota(jnp.int32, (BLOCK, 128), 1)
    result = jnp.dot(ordered[...], weight[...], preferred_element_type=jnp.float32)
    for k in range(4):
        part = result[k * BLOCK : (k + 1) * BLOCK, :]
        total = square[pl.ds(starts[k], BLOCK), :]
        if k % 2 == 0:
            keep_x[k // 2, :, :HALF] = part[:, :HALF]
            keep_x[k // 2, :, HALF:] = jnp.where(lane == 0, total, 0.0)
            keep_y[k // 2] = part[:, HALF:]
        else:
            send_x[k // 2, :, :HALF] = part[:, :HALF].astype(jnp.bfloat16)
            send_x[k // 2, :, HALF:] = pieces(total, lane)
            send_y[k // 2] = part[:, HALF:].astype(jnp.bfloat16)


def chip_kernel(keep, came, keep_out, send_out):
    keep_out[...] = keep[0] + came[0].astype(jnp.float32)
    leaving = keep[1] + came[1].astype(jnp.float32)
    send_out[:, :HALF] = leaving[:, :HALF].astype(jnp.bfloat16)
    if leaving.shape[1] > HALF:
        lane = lax.broadcasted_iota(jnp.int32, (BLOCK, 128), 1)
        total = jnp.sum(leaving[:, HALF:], axis=1, keepdims=True)
        send_out[:, HALF:] = pieces(jnp.broadcast_to(total, (BLOCK, 128)), lane)


def first_kernel(keep, came, rows, out, scale_out):
    total = keep[...] + came[...].astype(jnp.float32)
    square = jnp.sum(total[:, HALF:], axis=1, keepdims=True)
    scale = lax.rsqrt(square * (1.0 / INNER) + epsilon)
    scale_out[...] = jnp.broadcast_to(scale, (BLOCK, 128))
    wide = rows[0, 0, :, :HALF].astype(jnp.float32)
    out[...] = (wide + total[:, :HALF] * scale).astype(jnp.bfloat16)


def second_kernel(keep, came, rows, scale, out):
    total = keep[...] + came[...].astype(jnp.float32)
    wide = rows[0, 0, :, HALF:].astype(jnp.float32)
    out[...] = (wide + total * scale[:, :1]).astype(jnp.bfloat16)


VMEM = pl.BlockSpec(memory_space=pltpu.VMEM)
SMEM = pl.BlockSpec(memory_space=pltpu.SMEM)


def called(kernel, outs, scratch, scalars, *arrays):
    return pl.pallas_call(
        kernel,
        out_shape=outs,
        in_specs=[SMEM] * len(scalars) + [VMEM] * len(arrays),
        out_specs=jax.tree.map(lambda _: VMEM, outs),
        scratch_shapes=scratch,
        compiler_params=pltpu.CompilerParams(vmem_limit_bytes=40 * 1024 * 1024),
    )(*scalars, *arrays)


def swapped(x, axis):
    return lax.ppermute(x, axis, [(0, 1), (1, 0)])


def both_of(mine, theirs, index):
    first = jnp.where(index == 0, mine, theirs)
    second = jnp.where(index == 0, theirs, mine)
    return jnp.stack([first, second])


def shards(
    stream,
    norm_gain,
    w_xbc,
    w_dt,
    conv_weight,
    conv_bias,
    dt_bias,
    decay_rate,
    skip_weight,
    inner_gain,
    w_out,
):
    par, core = lax.axis_index("par"), lax.axis_index("core")
    group = par * 2 + core
    place = lax.axis_index("dp") * 2 + lax.axis_index("blk")
    where = jnp.stack([place, 1 - 2 * core, group, par, core]).astype(jnp.int32)

    out_chunks = gathered(w_out[0], 1)
    xbc, dtw = w_xbc[0], w_dt[0]
    inner = xbc[:, :INNER].reshape(40, 2, 4, 320).transpose(2, 0, 1, 3).reshape(4, 40, LOCAL)
    shared = jnp.broadcast_to(xbc[None, :, INNER:], (4, 40, 2 * STATE))
    steps = dtw.reshape(40, 2, 4, 5).transpose(2, 0, 1, 3).reshape(4, 40, LOCAL_HEADS)
    steps = jnp.pad(steps, ((0, 0), (0, 0), (0, 128 - LOCAL_HEADS)))
    packed = jnp.concatenate([inner, shared, steps], axis=2)
    classes = lax.all_to_all(packed, ("par", "core"), 0, 0).reshape(160, WIDE)
    in_chunks = gathered(classes, 0)

    rows_in = stream[0, 0]
    wide = rows_in.astype(jnp.float32)
    mean_square = jnp.mean(wide * wide, axis=-1, keepdims=True)
    normed = (wide * lax.rsqrt(mean_square + epsilon) * norm_gain[0]).astype(jnp.bfloat16)
    feature = lax.broadcasted_iota(jnp.int32, (D, D), 0)
    target = lax.broadcasted_iota(jnp.int32, (D, D), 1)
    source = (target // 640) * 640 + (target // 40 % 4) * 160 + (target // 160 % 4) * 40 + target % 40
    select = (feature == source).astype(jnp.bfloat16)
    normed = jnp.dot(normed, select, preferred_element_type=jnp.float32).astype(jnp.bfloat16)
    pair = both_of(normed, swapped(normed, "par"), par)
    quad = both_of(pair, swapped(pair, "core"), core)
    rows = quad.transpose(1, 0, 2, 3).reshape(ROWS, D)
    halo = lax.ppermute(rows[ROWS - 8 :], "blk", [(0, 1)])

    f32, bf16 = jnp.float32, jnp.bfloat16
    y_local, c_rows, grown, state = called(
        mix_kernel,
        (
            jax.ShapeDtypeStruct((ROWS, LOCAL), f32),
            jax.ShapeDtypeStruct((ROWS, STATE), bf16),
            jax.ShapeDtypeStruct((ROWS, LOCAL), f32),
            jax.ShapeDtypeStruct((STATE, LOCAL), bf16),
        ),
        [pltpu.VMEM((D, WIDE), bf16), pltpu.VMEM((ROWS + 8, TAPPED), f32)],
        (where,),
        rows,
        halo,
        conv_weight,
        conv_bias,
        dt_bias,
        decay_rate,
        skip_weight,
        *in_chunks,
    )
    arriving = lax.ppermute(state, "blk", [(0, 1)])

    shape = jax.ShapeDtypeStruct
    wide = HALF + 128
    keep_x, send_x, keep_y, send_y = called(
        out_kernel,
        (
            shape((2, BLOCK, wide), f32),
            shape((2, BLOCK, wide), bf16),
            shape((2, BLOCK, HALF), f32),
            shape((2, BLOCK, HALF), bf16),
        ),
        [
            pltpu.VMEM((LOCAL, D), bf16),
            pltpu.VMEM((ROWS, LOCAL), bf16),
            pltpu.VMEM((ROWS, 128), f32),
            pltpu.VMEM((ROWS, LOCAL), bf16),
        ],
        (where,),
        y_local,
        c_rows,
        grown,
        arriving,
        inner_gain,
        *out_chunks,
    )
    came_x, came_y = swapped(send_x, "core"), swapped(send_y, "core")
    keep_x, send_x = called(
        chip_kernel, (shape((BLOCK, wide), f32), shape((BLOCK, wide), bf16)), [], (), keep_x, came_x
    )
    came_x = swapped(send_x, "par")
    keep_y, send_y = called(
        chip_kernel, (shape((BLOCK, HALF), f32), shape((BLOCK, HALF), bf16)), [], (), keep_y, came_y
    )
    came_y = swapped(send_y, "par")
    next_x, scale = called(
        first_kernel,
        (shape((BLOCK, HALF), bf16), shape((BLOCK, 128), f32)),
        [],
        (),
        keep_x,
        came_x,
        stream,
    )
    next_y = called(
        second_kernel, shape((BLOCK, HALF), bf16), [], (), keep_y, came_y, stream, scale
    )
    onward = [(i, (i + 1) % 16) for i in range(16)]
    moved_x = lax.ppermute(next_x, "section", onward)
    moved_y = lax.ppermute(next_y, "section", onward)
    moved = jnp.concatenate([moved_x, moved_y], axis=1)
    return moved[None, None]


def solution(mesh):
    torus = Mesh(
        mesh.devices.reshape(mesh.shape["section"], 2, 2, 2, mesh.shape["dp"]),
        ("section", "blk", "par", "core", "dp"),
    )
    return jax.shard_map(
        shards,
        mesh=torus,
        in_specs=(
            P("section", "dp", SEQ, None),
            P("section", None),
            P("section", SEQ_DP, None),
            P("section", SEQ_DP, None),
            P("section", None, None),
            P("section", None),
            P("section", None),
            P("section", None),
            P("section", None),
            P("section", None),
            P("section", SEQ_DP, None),
        ),
        out_specs=P("section", "dp", SEQ, None),
        check_vma=False,
    )
```

```python
import jax
import jax.numpy as jnp
from jax import lax
from jax.experimental import pallas as pl
from jax.experimental.pallas import tpu as pltpu
from jax.sharding import Mesh
from jax.sharding import PartitionSpec as P

HEADS = 40
HEAD_DIM = 64
STATE = 64
CONV = 4
BLOCK = 128
INNER = 2560
D = 1280
SEQ = ("blk", "par", "core")
SEQ_DP = ("blk", "par", "core", "dp")
RING = ("blk", "core", "dp")
epsilon = 1e-05
LOCAL_HEADS = 10
LOCAL = LOCAL_HEADS * HEAD_DIM
TAPPED = LOCAL + 2 * STATE
WIDE = TAPPED + 128
ROWS = 512
PIECE = ROWS // BLOCK
HALF = D // 2


def ring_index(place, core):
    place = place % 8
    return (place % 2) * 8 + core * 4 + place // 2


def shifted(x, by):
    pairs = []
    for i in range(8):
        pairs.append((ring_index(i, 0), ring_index(i + by, 0)))
        pairs.append((ring_index(i, 1), ring_index(i - by, 1)))
    return lax.ppermute(x, RING, pairs)


def gathered(x, cut):
    up, down = x, x
    out = [x]
    for _ in range(1, 4):
        up, down = shifted(up, 1), shifted(down, -1)
        out += [up, down]
    half = x.shape[cut] // 2
    first = lax.slice_in_dim(up, 0, half, axis=cut)
    second = lax.slice_in_dim(down, half, 2 * half, axis=cut)
    out += [shifted(first, 1), shifted(second, -1)]
    return out


OFFSETS = (0, -1, 1, -2, 2, -3, 3, 4, 4)


def slot_of(place, offset):
    there = (place + offset + 8) % 8
    return (there % 2) * 4 + there // 2


def fill(where, chunks, scratch, cut):
    rows = chunks[0].shape[0]
    place, sign = where[0], where[1]
    for k in range(7):
        at = pl.multiple_of(slot_of(place, OFFSETS[k] * sign) * rows, 16)
        scratch[pl.ds(at, rows), :] = chunks[k][...]
    at = slot_of(place, 4) * rows
    if cut == 0:
        half = rows // 2
        scratch[pl.ds(pl.multiple_of(at, 16), half), :] = chunks[7][...]
        scratch[pl.ds(pl.multiple_of(at + half, 16), half), :] = chunks[8][...]
    else:
        half = chunks[7].shape[1]
        at = pl.multiple_of(at, 16)
        scratch[pl.ds(at, rows), :half] = chunks[7][...]
        scratch[pl.ds(at, rows), half:] = chunks[8][...]


def exact_dot(a, b):
    return jnp.dot(a, b, preferred_element_type=jnp.float32, precision=lax.Precision.HIGHEST)


def spread(per_head):
    rows = per_head.shape[0]
    left = lax.broadcasted_iota(jnp.int32, (rows, 128), 1) < HEAD_DIM
    pairs = []
    for p in range(LOCAL_HEADS // 2):
        first = jnp.broadcast_to(per_head[:, 2 * p : 2 * p + 1], (rows, 128))
        second = jnp.broadcast_to(per_head[:, 2 * p + 1 : 2 * p + 2], (rows, 128))
        pairs.append(jnp.where(left, first, second))
    return jnp.concatenate(pairs, axis=1)


def class_columns(x, group, width):
    found = None
    for g in range(4):
        piece = jnp.concatenate(
            [x[:, g * width : (g + 1) * width], x[:, (g + 4) * width : (g + 5) * width]], axis=1
        )
        found = piece if found is None else jnp.where(group == g, piece, found)
    return found


def class_heads(x, group, width, lanes):
    head = lax.broadcasted_iota(jnp.int32, (HEADS, lanes), 0)
    local = lax.broadcasted_iota(jnp.int32, (HEADS, lanes), 1) // width
    wanted = jnp.where(local < 5, group * 5 + local, 15 + group * 5 + local)
    select = jnp.logical_and(local < LOCAL_HEADS, head == wanted)
    return exact_dot(x, select.astype(jnp.float32))


def prep_kernel(where, all_taps, all_bias, all_dt_bias, all_rate, all_skip, all_gain, out):
    group = where[2]
    out[0:4, :LOCAL] = class_columns(all_taps[0], group, 320)
    out[0:4, LOCAL:] = all_taps[0, :, INNER:]
    out[4:5, :LOCAL] = class_columns(all_bias[...], group, 320)
    out[4:5, LOCAL:] = all_bias[:, INNER:]
    out[5:6, :LOCAL] = class_heads(all_skip[...], group, HEAD_DIM, LOCAL)
    out[6:7, :LOCAL] = class_columns(all_gain[...], group, 320)
    out[7:8, :128] = class_heads(all_dt_bias[...], group, 1, 128)
    out[8:9, :128] = class_heads(all_rate[...], group, 1, 128)


def mix_kernel(where, rows, halo, params, *rest):
    chunks, (y_out, c_out, grown_out, state_out, weight, raw) = rest[:9], rest[9:]
    fill(where, chunks, weight, 0)
    taps = params[0:4, :]
    bias = params[4:5, :]
    skip = params[5:6, :LOCAL]
    dt_bias = params[7:8, :128]
    rate = params[8:9, :128]
    projected = jnp.dot(rows[...], weight[...], preferred_element_type=jnp.float32)
    before = jnp.dot(halo[...], weight[:, :TAPPED], preferred_element_type=jnp.float32)
    raw[:8, :] = before.astype(jnp.bfloat16).astype(jnp.float32)
    raw[8:, :] = projected[:, :TAPPED].astype(jnp.bfloat16).astype(jnp.float32)
    shift = projected[:, TAPPED:] + dt_bias
    dt_all = jnp.maximum(shift, 0.0) + jnp.log1p(jnp.exp(-jnp.abs(shift)))
    row_id = lax.broadcasted_iota(jnp.int32, (BLOCK, BLOCK), 0)
    col_id = lax.broadcasted_iota(jnp.int32, (BLOCK, BLOCK), 1)
    causal = row_id >= col_id
    lower = causal.astype(jnp.float32)
    left = col_id < HEAD_DIM
    state = jnp.zeros((STATE, LOCAL), jnp.float32)
    decayed = jnp.ones((1, LOCAL), jnp.float32)
    for n in range(PIECE):
        at = n * BLOCK
        conv = bias + taps[0:1, :] * raw[at + 5 : at + 5 + BLOCK, :]
        for k in range(1, CONV):
            conv = conv + taps[k : k + 1, :] * raw[at + 5 + k : at + 5 + k + BLOCK, :]
        xbc = (conv / (1.0 + jnp.exp(-conv))).astype(jnp.bfloat16)
        values = xbc[:, :LOCAL]
        both = xbc[:, LOCAL:]
        b_rows, c_rows = both[:, :STATE], both[:, STATE:]
        dt = dt_all[at : at + BLOCK, :]
        cum = exact_dot(lower, -dt * rate)
        cum_t, dt_t = cum.T, dt.T
        scores = lax.dot_general(
            c_rows, b_rows, (((1,), (1,)), ((), ())), preferred_element_type=jnp.float32
        )
        scores = jnp.where(causal, scores, 0.0)
        intra = []
        for p in range(LOCAL_HEADS // 2):
            mixes = []
            for h in (2 * p, 2 * p + 1):
                lag = cum[:, h : h + 1] - cum_t[h : h + 1, :]
                weights = jnp.exp(jnp.minimum(lag, 0.0))
                mixes.append((scores * weights * dt_t[h : h + 1, :]).astype(jnp.bfloat16))
            pair = values[:, 128 * p : 128 * p + 128]
            none = jnp.zeros_like(pair)
            stacked = jnp.concatenate(
                [jnp.where(left, pair, none), jnp.where(left, none, pair)], axis=0
            )
            intra.append(
                jnp.dot(
                    jnp.concatenate(mixes, axis=1), stacked, preferred_element_type=jnp.float32
                )
            )
        wide = values.astype(jnp.float32)
        tail = spread(jnp.exp(cum[BLOCK - 1 :, :] - cum) * dt)
        growth = spread(jnp.exp(cum))
        scaled = (wide * tail).astype(jnp.bfloat16)
        local = jnp.concatenate(intra, axis=1) + skip * wide
        if n > 0:
            local = local + growth * exact_dot(c_rows.astype(jnp.float32), state)
        y_out[at : at + BLOCK, :] = local
        c_out[at : at + BLOCK, :] = c_rows
        grown_out[at : at + BLOCK, :] = growth * decayed
        summary = lax.dot_general(
            b_rows, scaled, (((0,), (0,)), ((), ())), preferred_element_type=jnp.float32
        )
        total = growth[BLOCK - 1 :, :]
        state = total * state + summary
        decayed = decayed * total
    state_out[...] = state.astype(jnp.bfloat16)


def pieces(square, lane):
    high = square.astype(jnp.bfloat16).astype(jnp.float32)
    middle = (square - high).astype(jnp.bfloat16).astype(jnp.float32)
    low = square - high - middle
    split = jnp.where(lane == 0, high, jnp.where(lane == 1, middle, jnp.where(lane == 2, low, 0.0)))
    return split.astype(jnp.bfloat16)


def out_kernel(where, y_in, c_in, grown, arriving, params, *rest):
    chunks, (keep_x, send_x, keep_y, send_y, weight, act, square, ordered) = rest[:9], rest[9:]
    fill(where, chunks, weight, 1)
    gain = params[6:7, :LOCAL]
    y = y_in[...] + grown[...] * jnp.dot(
        c_in[...], arriving[...], preferred_element_type=jnp.float32
    )
    act[...] = (y * gain).astype(jnp.bfloat16)
    square[...] = jnp.broadcast_to(jnp.sum(y * y, axis=1, keepdims=True), (ROWS, 128))
    par, core = where[3], where[4]
    starts = []
    for p in (par, 1 - par):
        for c in (core, 1 - core):
            starts.append(pl.multiple_of((p * 2 + c) * BLOCK, BLOCK))
    for k in range(4):
        ordered[k * BLOCK : (k + 1) * BLOCK, :] = act[pl.ds(starts[k], BLOCK), :]
    lane = lax.broadcasted_iota(jnp.int32, (BLOCK, 128), 1)
    result = jnp.dot(ordered[...], weight[...], preferred_element_type=jnp.float32)
    for k in range(4):
        part = result[k * BLOCK : (k + 1) * BLOCK, :]
        total = square[pl.ds(starts[k], BLOCK), :]
        if k % 2 == 0:
            keep_x[k // 2, :, :HALF] = part[:, :HALF]
            keep_x[k // 2, :, HALF:] = jnp.where(lane == 0, total, 0.0)
            keep_y[k // 2] = part[:, HALF:]
        else:
            send_x[k // 2, :, :HALF] = part[:, :HALF].astype(jnp.bfloat16)
            send_x[k // 2, :, HALF:] = pieces(total, lane)
            send_y[k // 2] = part[:, HALF:].astype(jnp.bfloat16)


def chip_kernel(keep, came, keep_out, send_out):
    keep_out[...] = keep[0] + came[0].astype(jnp.float32)
    leaving = keep[1] + came[1].astype(jnp.float32)
    send_out[:, :HALF] = leaving[:, :HALF].astype(jnp.bfloat16)
    if leaving.shape[1] > HALF:
        lane = lax.broadcasted_iota(jnp.int32, (BLOCK, 128), 1)
        total = jnp.sum(leaving[:, HALF:], axis=1, keepdims=True)
        send_out[:, HALF:] = pieces(jnp.broadcast_to(total, (BLOCK, 128)), lane)


def first_kernel(keep, came, rows, out, scale_out):
    total = keep[...] + came[...].astype(jnp.float32)
    square = jnp.sum(total[:, HALF:], axis=1, keepdims=True)
    scale = lax.rsqrt(square * (1.0 / INNER) + epsilon)
    scale_out[...] = jnp.broadcast_to(scale, (BLOCK, 128))
    wide = rows[:, :HALF].astype(jnp.float32)
    out[...] = (wide + total[:, :HALF] * scale).astype(jnp.bfloat16)


def second_kernel(keep, came, rows, scale, first, out):
    total = keep[...] + came[...].astype(jnp.float32)
    wide = rows[:, HALF:].astype(jnp.float32)
    out[0, 0, :, :HALF] = first[...]
    out[0, 0, :, HALF:] = (wide + total * scale[:, :1]).astype(jnp.bfloat16)


VMEM = pl.BlockSpec(memory_space=pltpu.VMEM)
SMEM = pl.BlockSpec(memory_space=pltpu.SMEM)


def called(kernel, outs, scratch, scalars, *arrays):
    return pl.pallas_call(
        kernel,
        out_shape=outs,
        in_specs=[SMEM] * len(scalars) + [VMEM] * len(arrays),
        out_specs=jax.tree.map(lambda _: VMEM, outs),
        scratch_shapes=scratch,
        compiler_params=pltpu.CompilerParams(vmem_limit_bytes=40 * 1024 * 1024),
    )(*scalars, *arrays)


def swapped(x, axis):
    return lax.ppermute(x, axis, [(0, 1), (1, 0)])


def onward(x):
    return lax.ppermute(x, "section", [(i, (i + 1) % 16) for i in range(16)])


def both_of(mine, theirs, index):
    first = jnp.where(index == 0, mine, theirs)
    second = jnp.where(index == 0, theirs, mine)
    return jnp.stack([first, second])


def shards(
    stream,
    norm_gain,
    w_xbc,
    w_dt,
    conv_weight,
    conv_bias,
    dt_bias,
    decay_rate,
    skip_weight,
    inner_gain,
    w_out,
):
    par, core = lax.axis_index("par"), lax.axis_index("core")
    group = par * 2 + core
    place = lax.axis_index("dp") * 2 + lax.axis_index("blk")
    where = jnp.stack([place, 1 - 2 * core, group, par, core]).astype(jnp.int32)

    out_chunks = gathered(onward(w_out[0]), 1)
    raw = onward(jnp.concatenate([w_xbc[0], w_dt[0]], axis=1))
    xbc, dtw = raw[:, : INNER + 2 * STATE], raw[:, INNER + 2 * STATE :]
    inner = xbc[:, :INNER].reshape(40, 2, 4, 320).transpose(2, 0, 1, 3).reshape(4, 40, LOCAL)
    shared = jnp.broadcast_to(xbc[None, :, INNER:], (4, 40, 2 * STATE))
    steps = dtw.reshape(40, 2, 4, 5).transpose(2, 0, 1, 3).reshape(4, 40, LOCAL_HEADS)
    steps = jnp.pad(steps, ((0, 0), (0, 0), (0, 128 - LOCAL_HEADS)))
    packed = jnp.concatenate([inner, shared, steps], axis=2)
    classes = lax.all_to_all(packed, ("par", "core"), 0, 0).reshape(160, WIDE)
    in_chunks = gathered(classes, 0)

    rows_in = stream[0, 0]
    wide = rows_in.astype(jnp.float32)
    mean_square = jnp.mean(wide * wide, axis=-1, keepdims=True)
    normed = (wide * lax.rsqrt(mean_square + epsilon) * norm_gain[0]).astype(jnp.bfloat16)
    feature = lax.broadcasted_iota(jnp.int32, (D, D), 0)
    target = lax.broadcasted_iota(jnp.int32, (D, D), 1)
    source = (target // 640) * 640 + (target // 40 % 4) * 160 + (target // 160 % 4) * 40 + target % 40
    select = (feature == source).astype(jnp.bfloat16)
    normed = jnp.dot(normed, select, preferred_element_type=jnp.float32).astype(jnp.bfloat16)
    normed = onward(normed)
    pair = both_of(normed, swapped(normed, "par"), par)
    quad = both_of(pair, swapped(pair, "core"), core)
    rows = quad.transpose(1, 0, 2, 3).reshape(ROWS, D)
    halo = lax.ppermute(rows[ROWS - 8 :], "blk", [(0, 1)])

    f32, bf16 = jnp.float32, jnp.bfloat16
    params = called(
        prep_kernel,
        jax.ShapeDtypeStruct((16, TAPPED), f32),
        [],
        (where,),
        conv_weight,
        conv_bias,
        dt_bias,
        decay_rate,
        skip_weight,
        inner_gain,
    )
    params = onward(params)
    residual = onward(rows_in)
    y_local, c_rows, grown, state = called(
        mix_kernel,
        (
            jax.ShapeDtypeStruct((ROWS, LOCAL), f32),
            jax.ShapeDtypeStruct((ROWS, STATE), bf16),
            jax.ShapeDtypeStruct((ROWS, LOCAL), f32),
            jax.ShapeDtypeStruct((STATE, LOCAL), bf16),
        ),
        [pltpu.VMEM((D, WIDE), bf16), pltpu.VMEM((ROWS + 8, TAPPED), f32)],
        (where,),
        rows,
        halo,
        params,
        *in_chunks,
    )
    arriving = lax.ppermute(state, "blk", [(0, 1)])

    shape = jax.ShapeDtypeStruct
    wide = HALF + 128
    keep_x, send_x, keep_y, send_y = called(
        out_kernel,
        (
            shape((2, BLOCK, wide), f32),
            shape((2, BLOCK, wide), bf16),
            shape((2, BLOCK, HALF), f32),
            shape((2, BLOCK, HALF), bf16),
        ),
        [
            pltpu.VMEM((LOCAL, D), bf16),
            pltpu.VMEM((ROWS, LOCAL), bf16),
            pltpu.VMEM((ROWS, 128), f32),
            pltpu.VMEM((ROWS, LOCAL), bf16),
        ],
        (where,),
        y_local,
        c_rows,
        grown,
        arriving,
        params,
        *out_chunks,
    )
    came_x, came_y = swapped(send_x, "core"), swapped(send_y, "core")
    keep_x, send_x = called(
        chip_kernel, (shape((BLOCK, wide), f32), shape((BLOCK, wide), bf16)), [], (), keep_x, came_x
    )
    came_x = swapped(send_x, "par")
    keep_y, send_y = called(
        chip_kernel, (shape((BLOCK, HALF), f32), shape((BLOCK, HALF), bf16)), [], (), keep_y, came_y
    )
    came_y = swapped(send_y, "par")
    next_x, scale = called(
        first_kernel,
        (shape((BLOCK, HALF), bf16), shape((BLOCK, 128), f32)),
        [],
        (),
        keep_x,
        came_x,
        residual,
    )
    return called(
        second_kernel,
        shape((1, 1, BLOCK, D), bf16),
        [],
        (),
        keep_y,
        came_y,
        residual,
        scale,
        next_x,
    )


def solution(mesh):
    torus = Mesh(
        mesh.devices.reshape(mesh.shape["section"], 2, 2, 2, mesh.shape["dp"]),
        ("section", "blk", "par", "core", "dp"),
    )
    return jax.shard_map(
        shards,
        mesh=torus,
        in_specs=(
            P("section", "dp", SEQ, None),
            P("section", None),
            P("section", SEQ_DP, None),
            P("section", SEQ_DP, None),
            P("section", None, None),
            P("section", None),
            P("section", None),
            P("section", None),
            P("section", None),
            P("section", None),
            P("section", SEQ_DP, None),
        ),
        out_specs=P("section", "dp", SEQ, None),
        check_vma=False,
    )
```

```python
import jax
import jax.numpy as jnp
from jax import lax
from jax.experimental import pallas as pl
from jax.experimental.pallas import tpu as pltpu
from jax.sharding import Mesh
from jax.sharding import PartitionSpec as P

HEADS = 40
HEAD_DIM = 64
STATE = 64
CONV = 4
BLOCK = 128
INNER = 2560
D = 1280
SEQ = ("blk", "par", "core")
SEQ_DP = ("blk", "par", "core", "dp")
RING = ("blk", "core", "dp")
epsilon = 1e-05
LOCAL_HEADS = 10
LOCAL = LOCAL_HEADS * HEAD_DIM
TAPPED = LOCAL + 2 * STATE
WIDE = TAPPED + 128
ROWS = 512
PIECE = ROWS // BLOCK
HALF = D // 2


def ring_index(place, core):
    place = place % 8
    return (place % 2) * 8 + core * 4 + place // 2


def shifted(x, by):
    pairs = []
    for i in range(8):
        pairs.append((ring_index(i, 0), ring_index(i + by, 0)))
        pairs.append((ring_index(i, 1), ring_index(i - by, 1)))
    return lax.ppermute(x, RING, pairs)


def gathered(x, cut):
    up, down = x, x
    out = [x]
    for _ in range(1, 4):
        up, down = shifted(up, 1), shifted(down, -1)
        out += [up, down]
    half = x.shape[cut] // 2
    first = lax.slice_in_dim(up, 0, half, axis=cut)
    second = lax.slice_in_dim(down, half, 2 * half, axis=cut)
    out += [shifted(first, 1), shifted(second, -1)]
    return out


OFFSETS = (0, -1, 1, -2, 2, -3, 3, 4, 4)


def slot_of(place, offset):
    there = (place + offset + 8) % 8
    return (there % 2) * 4 + there // 2


def fill(where, chunks, scratch, cut):
    rows = chunks[0].shape[0]
    place, sign = where[0], where[1]
    for k in range(7):
        at = pl.multiple_of(slot_of(place, OFFSETS[k] * sign) * rows, 16)
        scratch[pl.ds(at, rows), :] = chunks[k][...]
    at = slot_of(place, 4) * rows
    if cut == 0:
        half = rows // 2
        scratch[pl.ds(pl.multiple_of(at, 16), half), :] = chunks[7][...]
        scratch[pl.ds(pl.multiple_of(at + half, 16), half), :] = chunks[8][...]
    else:
        half = chunks[7].shape[1]
        at = pl.multiple_of(at, 16)
        scratch[pl.ds(at, rows), :half] = chunks[7][...]
        scratch[pl.ds(at, rows), half:] = chunks[8][...]


def exact_dot(a, b):
    return jnp.dot(a, b, preferred_element_type=jnp.float32, precision=lax.Precision.HIGHEST)


def spread(per_head):
    rows = per_head.shape[0]
    left = lax.broadcasted_iota(jnp.int32, (rows, 128), 1) < HEAD_DIM
    pairs = []
    for p in range(LOCAL_HEADS // 2):
        first = jnp.broadcast_to(per_head[:, 2 * p : 2 * p + 1], (rows, 128))
        second = jnp.broadcast_to(per_head[:, 2 * p + 1 : 2 * p + 2], (rows, 128))
        pairs.append(jnp.where(left, first, second))
    return jnp.concatenate(pairs, axis=1)


def class_columns(x, group, width):
    found = None
    for g in range(4):
        piece = jnp.concatenate(
            [x[:, g * width : (g + 1) * width], x[:, (g + 4) * width : (g + 5) * width]], axis=1
        )
        found = piece if found is None else jnp.where(group == g, piece, found)
    return found


def class_heads(x, group, width, lanes):
    head = lax.broadcasted_iota(jnp.int32, (HEADS, lanes), 0)
    local = lax.broadcasted_iota(jnp.int32, (HEADS, lanes), 1) // width
    wanted = jnp.where(local < 5, group * 5 + local, 15 + group * 5 + local)
    select = jnp.logical_and(local < LOCAL_HEADS, head == wanted)
    return exact_dot(x, select.astype(jnp.float32))


def prep_kernel(where, all_taps, all_bias, all_dt_bias, all_rate, all_skip, all_gain, out):
    group = where[2]
    out[0:4, :LOCAL] = class_columns(all_taps[0], group, 320)
    out[0:4, LOCAL:] = all_taps[0, :, INNER:]
    out[4:5, :LOCAL] = class_columns(all_bias[...], group, 320)
    out[4:5, LOCAL:] = all_bias[:, INNER:]
    out[5:6, :LOCAL] = class_heads(all_skip[...], group, HEAD_DIM, LOCAL)
    out[6:7, :LOCAL] = class_columns(all_gain[...], group, 320)
    out[7:8, :128] = class_heads(all_dt_bias[...], group, 1, 128)
    out[8:9, :128] = class_heads(all_rate[...], group, 1, 128)


def mix_kernel(where, rows, halo, params, *rest):
    chunks, (y_out, c_out, grown_out, state_out, weight, raw) = rest[:9], rest[9:]
    fill(where, chunks, weight, 0)
    taps = params[0:4, :]
    bias = params[4:5, :]
    skip = params[5:6, :LOCAL]
    dt_bias = params[7:8, :128]
    rate = params[8:9, :128]
    projected = jnp.dot(rows[...], weight[...], preferred_element_type=jnp.float32)
    before = jnp.dot(halo[...], weight[:, :TAPPED], preferred_element_type=jnp.float32)
    raw[:8, :] = before.astype(jnp.bfloat16).astype(jnp.float32)
    raw[8:, :] = projected[:, :TAPPED].astype(jnp.bfloat16).astype(jnp.float32)
    shift = projected[:, TAPPED:] + dt_bias
    dt_all = jnp.maximum(shift, 0.0) + jnp.log1p(jnp.exp(-jnp.abs(shift)))
    row_id = lax.broadcasted_iota(jnp.int32, (BLOCK, BLOCK), 0)
    col_id = lax.broadcasted_iota(jnp.int32, (BLOCK, BLOCK), 1)
    causal = row_id >= col_id
    lower = causal.astype(jnp.float32)
    left = col_id < HEAD_DIM
    state = jnp.zeros((STATE, LOCAL), jnp.float32)
    decayed = jnp.ones((1, LOCAL), jnp.float32)
    for n in range(PIECE):
        at = n * BLOCK
        conv = bias + taps[0:1, :] * raw[at + 5 : at + 5 + BLOCK, :]
        for k in range(1, CONV):
            conv = conv + taps[k : k + 1, :] * raw[at + 5 + k : at + 5 + k + BLOCK, :]
        xbc = (conv / (1.0 + jnp.exp(-conv))).astype(jnp.bfloat16)
        values = xbc[:, :LOCAL]
        both = xbc[:, LOCAL:]
        b_rows, c_rows = both[:, :STATE], both[:, STATE:]
        dt = dt_all[at : at + BLOCK, :]
        cum = exact_dot(lower, -dt * rate)
        cum_t, dt_t = cum.T, dt.T
        scores = lax.dot_general(
            c_rows, b_rows, (((1,), (1,)), ((), ())), preferred_element_type=jnp.float32
        )
        scores = jnp.where(causal, scores, 0.0)
        intra = []
        for p in range(LOCAL_HEADS // 2):
            mixes = []
            for h in (2 * p, 2 * p + 1):
                lag = cum[:, h : h + 1] - cum_t[h : h + 1, :]
                weights = jnp.exp(jnp.minimum(lag, 0.0))
                mixes.append((scores * weights * dt_t[h : h + 1, :]).astype(jnp.bfloat16))
            pair = values[:, 128 * p : 128 * p + 128]
            none = jnp.zeros_like(pair)
            stacked = jnp.concatenate(
                [jnp.where(left, pair, none), jnp.where(left, none, pair)], axis=0
            )
            intra.append(
                jnp.dot(
                    jnp.concatenate(mixes, axis=1), stacked, preferred_element_type=jnp.float32
                )
            )
        wide = values.astype(jnp.float32)
        tail = spread(jnp.exp(cum[BLOCK - 1 :, :] - cum) * dt)
        growth = spread(jnp.exp(cum))
        scaled = (wide * tail).astype(jnp.bfloat16)
        local = jnp.concatenate(intra, axis=1) + skip * wide
        if n > 0:
            local = local + growth * exact_dot(c_rows.astype(jnp.float32), state)
        y_out[at : at + BLOCK, :] = local
        c_out[at : at + BLOCK, :] = c_rows
        grown_out[at : at + BLOCK, :] = growth * decayed
        summary = lax.dot_general(
            b_rows, scaled, (((0,), (0,)), ((), ())), preferred_element_type=jnp.float32
        )
        total = growth[BLOCK - 1 :, :]
        state = total * state + summary
        decayed = decayed * total
    state_out[...] = state.astype(jnp.bfloat16)


def pieces(square, lane):
    high = square.astype(jnp.bfloat16).astype(jnp.float32)
    middle = (square - high).astype(jnp.bfloat16).astype(jnp.float32)
    low = square - high - middle
    split = jnp.where(lane == 0, high, jnp.where(lane == 1, middle, jnp.where(lane == 2, low, 0.0)))
    return split.astype(jnp.bfloat16)


def out_kernel(where, y_in, c_in, grown, arriving, params, *rest):
    chunks, (keep_x, send_x, keep_y, send_y, weight, act, square, ordered) = rest[:9], rest[9:]
    fill(where, chunks, weight, 1)
    gain = params[6:7, :LOCAL]
    y = y_in[...] + grown[...] * jnp.dot(
        c_in[...], arriving[...], preferred_element_type=jnp.float32
    )
    act[...] = (y * gain).astype(jnp.bfloat16)
    square[...] = jnp.broadcast_to(jnp.sum(y * y, axis=1, keepdims=True), (ROWS, 128))
    par, core = where[3], where[4]
    starts = []
    for p in (par, 1 - par):
        for c in (core, 1 - core):
            starts.append(pl.multiple_of((p * 2 + c) * BLOCK, BLOCK))
    for k in range(4):
        ordered[k * BLOCK : (k + 1) * BLOCK, :] = act[pl.ds(starts[k], BLOCK), :]
    lane = lax.broadcasted_iota(jnp.int32, (BLOCK, 128), 1)
    result = jnp.dot(ordered[...], weight[...], preferred_element_type=jnp.float32)
    for k in range(4):
        part = result[k * BLOCK : (k + 1) * BLOCK, :]
        total = square[pl.ds(starts[k], BLOCK), :]
        if k % 2 == 0:
            keep_x[k // 2, :, :HALF] = part[:, :HALF]
            keep_x[k // 2, :, HALF:] = jnp.where(lane == 0, total, 0.0)
            keep_y[k // 2] = part[:, HALF:]
        else:
            send_x[k // 2, :, :HALF] = part[:, :HALF].astype(jnp.bfloat16)
            send_x[k // 2, :, HALF:] = pieces(total, lane)
            send_y[k // 2] = part[:, HALF:].astype(jnp.bfloat16)


def chip_kernel(keep, came, keep_out, send_out):
    keep_out[...] = keep[0] + came[0].astype(jnp.float32)
    leaving = keep[1] + came[1].astype(jnp.float32)
    send_out[:, :HALF] = leaving[:, :HALF].astype(jnp.bfloat16)
    if leaving.shape[1] > HALF:
        lane = lax.broadcasted_iota(jnp.int32, (BLOCK, 128), 1)
        total = jnp.sum(leaving[:, HALF:], axis=1, keepdims=True)
        send_out[:, HALF:] = pieces(jnp.broadcast_to(total, (BLOCK, 128)), lane)


def first_kernel(keep, came, rows, out, scale_out):
    total = keep[...] + came[...].astype(jnp.float32)
    square = jnp.sum(total[:, HALF:], axis=1, keepdims=True)
    scale = lax.rsqrt(square * (1.0 / INNER) + epsilon)
    scale_out[...] = jnp.broadcast_to(scale, (BLOCK, 128))
    wide = rows[0, 0, :, :HALF].astype(jnp.float32)
    out[...] = (wide + total[:, :HALF] * scale).astype(jnp.bfloat16)


def second_kernel(keep, came, rows, scale, out):
    total = keep[...] + came[...].astype(jnp.float32)
    wide = rows[0, 0, :, HALF:].astype(jnp.float32)
    out[...] = (wide + total * scale[:, :1]).astype(jnp.bfloat16)


VMEM = pl.BlockSpec(memory_space=pltpu.VMEM)
SMEM = pl.BlockSpec(memory_space=pltpu.SMEM)


def called(kernel, outs, scratch, scalars, *arrays):
    return pl.pallas_call(
        kernel,
        out_shape=outs,
        in_specs=[SMEM] * len(scalars) + [VMEM] * len(arrays),
        out_specs=jax.tree.map(lambda _: VMEM, outs),
        scratch_shapes=scratch,
        compiler_params=pltpu.CompilerParams(vmem_limit_bytes=40 * 1024 * 1024),
    )(*scalars, *arrays)


def swapped(x, axis):
    return lax.ppermute(x, axis, [(0, 1), (1, 0)])


def both_of(mine, theirs, index):
    first = jnp.where(index == 0, mine, theirs)
    second = jnp.where(index == 0, theirs, mine)
    return jnp.stack([first, second])


def shards(
    stream,
    norm_gain,
    w_xbc,
    w_dt,
    conv_weight,
    conv_bias,
    dt_bias,
    decay_rate,
    skip_weight,
    inner_gain,
    w_out,
):
    par, core = lax.axis_index("par"), lax.axis_index("core")
    group = par * 2 + core
    place = lax.axis_index("dp") * 2 + lax.axis_index("blk")
    where = jnp.stack([place, 1 - 2 * core, group, par, core]).astype(jnp.int32)

    out_chunks = gathered(w_out[0], 1)
    xbc, dtw = w_xbc[0], w_dt[0]
    inner = xbc[:, :INNER].reshape(40, 2, 4, 320).transpose(2, 0, 1, 3).reshape(4, 40, LOCAL)
    shared = jnp.broadcast_to(xbc[None, :, INNER:], (4, 40, 2 * STATE))
    steps = dtw.reshape(40, 2, 4, 5).transpose(2, 0, 1, 3).reshape(4, 40, LOCAL_HEADS)
    steps = jnp.pad(steps, ((0, 0), (0, 0), (0, 128 - LOCAL_HEADS)))
    packed = jnp.concatenate([inner, shared, steps], axis=2)
    classes = lax.all_to_all(packed, ("par", "core"), 0, 0).reshape(160, WIDE)
    in_chunks = gathered(classes, 0)

    rows_in = stream[0, 0]
    wide = rows_in.astype(jnp.float32)
    mean_square = jnp.mean(wide * wide, axis=-1, keepdims=True)
    normed = (wide * lax.rsqrt(mean_square + epsilon) * norm_gain[0]).astype(jnp.bfloat16)
    feature = lax.broadcasted_iota(jnp.int32, (D, D), 0)
    target = lax.broadcasted_iota(jnp.int32, (D, D), 1)
    source = (target // 640) * 640 + (target // 40 % 4) * 160 + (target // 160 % 4) * 40 + target % 40
    select = (feature == source).astype(jnp.bfloat16)
    normed = jnp.dot(normed, select, preferred_element_type=jnp.float32).astype(jnp.bfloat16)
    beside = swapped(normed, "par")
    pair = both_of(normed, beside, par)
    quad = both_of(pair, swapped(pair, "core"), core)
    rows = quad.transpose(1, 0, 2, 3).reshape(ROWS, D)
    halo = lax.ppermute(rows[ROWS - 8 :], "blk", [(0, 1)])

    f32, bf16 = jnp.float32, jnp.bfloat16
    params = called(
        prep_kernel,
        jax.ShapeDtypeStruct((16, TAPPED), f32),
        [],
        (where,),
        conv_weight,
        conv_bias,
        dt_bias,
        decay_rate,
        skip_weight,
        inner_gain,
    )
    y_local, c_rows, grown, state = called(
        mix_kernel,
        (
            jax.ShapeDtypeStruct((ROWS, LOCAL), f32),
            jax.ShapeDtypeStruct((ROWS, STATE), bf16),
            jax.ShapeDtypeStruct((ROWS, LOCAL), f32),
            jax.ShapeDtypeStruct((STATE, LOCAL), bf16),
        ),
        [pltpu.VMEM((D, WIDE), bf16), pltpu.VMEM((ROWS + 8, TAPPED), f32)],
        (where,),
        rows,
        halo,
        params,
        *in_chunks,
    )
    arriving = lax.ppermute(state, "blk", [(0, 1)])

    shape = jax.ShapeDtypeStruct
    wide = HALF + 128
    keep_x, send_x, keep_y, send_y = called(
        out_kernel,
        (
            shape((2, BLOCK, wide), f32),
            shape((2, BLOCK, wide), bf16),
            shape((2, BLOCK, HALF), f32),
            shape((2, BLOCK, HALF), bf16),
        ),
        [
            pltpu.VMEM((LOCAL, D), bf16),
            pltpu.VMEM((ROWS, LOCAL), bf16),
            pltpu.VMEM((ROWS, 128), f32),
            pltpu.VMEM((ROWS, LOCAL), bf16),
        ],
        (where,),
        y_local,
        c_rows,
        grown,
        arriving,
        params,
        *out_chunks,
    )
    came_x, came_y = swapped(send_x, "core"), swapped(send_y, "core")
    keep_x, send_x = called(
        chip_kernel, (shape((BLOCK, wide), f32), shape((BLOCK, wide), bf16)), [], (), keep_x, came_x
    )
    came_x = swapped(send_x, "par")
    keep_y, send_y = called(
        chip_kernel, (shape((BLOCK, HALF), f32), shape((BLOCK, HALF), bf16)), [], (), keep_y, came_y
    )
    came_y = swapped(send_y, "par")
    next_x, scale = called(
        first_kernel,
        (shape((BLOCK, HALF), bf16), shape((BLOCK, 128), f32)),
        [],
        (),
        keep_x,
        came_x,
        stream,
    )
    next_y = called(
        second_kernel, shape((BLOCK, HALF), bf16), [], (), keep_y, came_y, stream, scale
    )
    onward = [(i, (i + 1) % 16) for i in range(16)]
    moved_x = lax.ppermute(next_x, "section", onward)
    moved_y = lax.ppermute(next_y, "section", onward)
    moved = jnp.concatenate([moved_x, moved_y], axis=1)
    return moved[None, None]


def solution(mesh):
    torus = Mesh(
        mesh.devices.reshape(mesh.shape["section"], 2, 2, 2, mesh.shape["dp"]),
        ("section", "blk", "par", "core", "dp"),
    )
    return jax.shard_map(
        shards,
        mesh=torus,
        in_specs=(
            P("section", "dp", SEQ, None),
            P("section", None),
            P("section", SEQ_DP, None),
            P("section", SEQ_DP, None),
            P("section", None, None),
            P("section", None),
            P("section", None),
            P("section", None),
            P("section", None),
            P("section", None),
            P("section", SEQ_DP, None),
        ),
        out_specs=P("section", "dp", SEQ, None),
        check_vma=False,
    )
```
